128 devices in a mesh: dp: 8 (over y, x_hi), mp: 16 (over z, x_lo, core).
Axes of the slice: x: 4 (x_hi: 2, x_lo: 2; x = x_hi * 2 + x_lo), y: 4, z: 4, core: 2. Of those that a mesh axis runs over, the one named last changes fastest.
Arguments:
- emb_grad: bfloat16 [76032, 3584], P('mp', 'dp'), may hold values from -70 to 70
- emb_mom: bfloat16 [16, 8, 8, 594, 448], P('mp', None, 'dp'), may hold values from -0.29882812 to 0.29882812
- blk_grad: bfloat16 [2, 3584, 18944], P(None, 'dp', 'mp'), may hold values from -70 to 70
- blk_mom: bfloat16 [2, 16, 3584, 1184], P(None, None, ('dp', 'mp')), may hold values from -0.29882812 to 0.29882812
- tile_group: int32 [2, 16, 16], replicated, may hold values from 1 to 3
- clip_rms: float32 [4], replicated, may hold values from 0.05 to 80
Outputs:
- emb_update: bfloat16 [16, 8, 8, 594, 448], P('mp', None, 'dp')
- emb_moment: bfloat16 [16, 8, 8, 594, 448], P('mp', None, 'dp')
- blk_update: bfloat16 [2, 16, 3584, 1184], P(None, None, ('dp', 'mp'))
- blk_moment: bfloat16 [2, 16, 3584, 1184], P(None, None, ('dp', 'mp'))
The draws below stay inside these ranges and needn't reach their ends.
All inputs are finite; a program needn't handle non-finite values.
Results may differ from the reference program's by a relative error of at most 0.001.
Values may be sent and summed in bfloat16 or wider, within the bound.
No kernel may reach another device: no remote copies, remote signals or barrier semaphores. Data moves between devices by JAX's collectives and lax.ppermute only.
A program may use at most 128 MiB of HBM per device.

```python
import math
import jax
import jax.numpy as jnp
from jax import lax

D = 3584
FF = 18944
V = 76032
G = 4
RB = 2
ID_ROWS = 16
EMB_OWN = 594
DC = 448
FFC = 1184
N_DP = 8
N_MP = 16


def rough_scales(key, count, top):
    return jnp.exp(jax.random.uniform(key, (count,), jnp.float32) * math.log(top))


def block_scales(key, blocks, width, top):
    place = jnp.arange(blocks, dtype=jnp.float32) / float(max(blocks - 1, 1))
    unit = jax.random.uniform(key, (blocks,), jnp.float32)
    scales = jnp.exp((0.5 * place + 0.5 * unit) * math.log(top))
    return jnp.repeat(scales, width, total_repeat_length=blocks * width)


def draw_emb_grad(key, part):
    first_key = jax.random.fold_in(key, 0)
    second_key = jax.random.fold_in(key, 1)
    fourth_key = jax.random.fold_in(key, 3)
    fifth_key = jax.random.fold_in(key, 4)
    column_blocks = D // DC
    row_blocks = V // (EMB_OWN * column_blocks)
    rowscale = rough_scales(second_key, V, 10.0) * block_scales(fourth_key, row_blocks, V // row_blocks, 10.0)
    colscale = block_scales(fifth_key, column_blocks, DC, 3.0)
    values = jnp.clip(jax.random.normal(first_key, (V, D), jnp.float32), -4.0, 4.0) * 0.058
    values = values * rowscale[:, None] * colscale[None, :]
    return values.astype(jnp.bfloat16)


def draw_blk_grad(key, part):
    first_key = jax.random.fold_in(jax.random.fold_in(key, 7), 0)
    second_key = jax.random.fold_in(jax.random.fold_in(key, 7), 1)
    fourth_key = jax.random.fold_in(jax.random.fold_in(key, 7), 3)
    fifth_key = jax.random.fold_in(jax.random.fold_in(key, 7), 4)
    row_blocks = D // DC
    column_blocks = FF // FFC
    rowscale = rough_scales(second_key, D, 10.0) * block_scales(fourth_key, row_blocks, DC, 3.0)
    colscale = block_scales(fifth_key, column_blocks, FFC, 10.0)
    values = jnp.clip(jax.random.normal(first_key, (2, D, FF), jnp.float32), -4.0, 4.0) * 0.058
    values = values * rowscale[None, :, None] * colscale[None, None, :]
    return values.astype(jnp.bfloat16)


def draw_clip_rms(key, part):
    first_key, second_key = jax.random.split(jax.random.fold_in(key, 11))
    order = jax.random.permutation(first_key, G)
    lower = order < G // 2
    unit = jax.random.uniform(second_key, (G,), jnp.float32)
    small_values = 0.05 * jnp.exp(unit * math.log(10.0))
    large_values = 40.0 * jnp.exp(unit * math.log(2.0))
    return jnp.where(lower, small_values, large_values).astype(jnp.float32)


def set_ends(entries, stream_key, low, high):
    spot = [jax.random.randint(jax.random.fold_in(stream_key, axis), (), 0, length) for axis, length in enumerate(entries.shape)]
    longest = entries.shape.index(max(entries.shape))
    neighbour = spot[:longest] + [(spot[longest] + 1) % entries.shape[longest]] + spot[longest + 1:]
    return entries.at[tuple(spot)].set(low).at[tuple(neighbour)].set(high)


def block_scale(stream_key, dims, cuts, least, largest):
    def one(position, shards_of):
        steps = jax.random.uniform(jax.random.fold_in(jax.random.fold_in(stream_key, 6), position), (shards_of,), jnp.float32, least / len(cuts), largest / len(cuts))
        return jnp.repeat(jnp.exp(steps), dims[position] // shards_of).reshape((-1,) + (1,) * (len(dims) - position - 1))

    loudness = one(*cuts[0])
    for cut in cuts[1:]:
        loudness = loudness * one(*cut)
    return loudness


def noise(rng, extent, spread, most, cuts=(), kind=jnp.bfloat16):
    factor_of = block_scale(rng, extent, cuts, -0.22, 0.18) if cuts else 1.0
    values = jax.random.normal(rng, extent, jnp.float32) * spread * factor_of
    return jnp.minimum(jnp.maximum(values, -most), most).astype(kind)


def setup_inputs(seed: int = 0) -> dict:
    streams_of = jax.random.split(jax.random.key(seed), 7)
    emb_grad = draw_emb_grad(jax.random.fold_in(streams_of[6], 71), 0)
    emb_mom = noise(streams_of[1], (N_MP, N_DP, N_DP, EMB_OWN, DC), 0.05, 0.29882812, ((0, 16), (2, 8)))
    blk_grad = draw_blk_grad(jax.random.fold_in(streams_of[6], 71), 0)
    blk_mom = noise(streams_of[3], (2, N_MP, D, FFC), 0.05, 0.29882812, ((2, 128),))
    tile_group = set_ends(jax.random.randint(streams_of[4], (2, ID_ROWS, N_MP), 1, G), jax.random.fold_in(streams_of[4], 1), 1, G - 1).astype(jnp.int32)
    clip_rms = draw_clip_rms(jax.random.fold_in(streams_of[6], 71), 0)
    return {"emb_grad": emb_grad, "emb_mom": emb_mom, "blk_grad": blk_grad, "blk_mom": blk_mom, "tile_group": tile_group, "clip_rms": clip_rms}


beta_first = 0.9
beta_second = 0.99
temper = 0.05
epsilon = 1e-06

def lion_step(clipped, moment):
    moment = moment.astype(jnp.float32)
    update = jnp.tanh((beta_first * moment + (1.0 - beta_first) * clipped) / temper).astype(jnp.bfloat16)
    new_moment = (beta_second * moment + (1.0 - beta_second) * clipped).astype(jnp.bfloat16)
    return (update, new_moment)

def square_sum(pieces):
    return jnp.sum(jnp.square(pieces.astype(jnp.float32)))

def reference(emb_grad, emb_mom, blk_grad, blk_mom, tile_group, clip_rms):
    block_height = D // (RB * N_DP)
    block_cols = FF // N_MP
    labels = jnp.arange(G, dtype=jnp.int32)
    first = (labels == 0).astype(jnp.float32)
    onehot = (tile_group[..., None] == labels).astype(jnp.float32)
    spans = emb_grad.reshape(N_MP * N_DP, EMB_OWN, D)
    emb_squares = jnp.sum(lax.map(square_sum, spans))
    block = blk_grad.astype(jnp.float32).reshape(2, RB * N_DP, block_height, N_MP, block_cols)
    block_squares = lax.optimization_barrier(jnp.sum(jnp.square(block), axis=(2, 4)))
    totals = lax.optimization_barrier(jnp.sum(block_squares[..., None] * onehot, axis=(0, 1, 2))) + emb_squares * first
    counts = lax.optimization_barrier(jnp.sum(onehot, axis=(0, 1, 2))) * float(block_height * block_cols) + first * float(V * D)
    root_mean = jnp.sqrt(totals / jnp.maximum(counts, 1.0))
    factor = jnp.minimum(1.0, clip_rms / (root_mean + epsilon))
    moments = jnp.transpose(emb_mom, (0, 2, 3, 1, 4)).reshape(N_MP * N_DP, EMB_OWN, D)

    def embed_span(paired):
        return lion_step(paired[0].astype(jnp.float32) * factor[0], paired[1])
    emb_update, emb_moment = lax.map(embed_span, (spans, moments))

    def to_owner(values):
        return jnp.transpose(values.reshape(N_MP, N_DP, EMB_OWN, N_DP, D // N_DP), (0, 3, 1, 2, 4))
    block_factor = lax.optimization_barrier(jnp.sum(onehot * factor, axis=-1))
    clipped = (block * block_factor[:, :, None, :, None]).reshape(2, D, N_MP, block_cols)
    blk_plain = jnp.transpose(blk_mom, (0, 2, 1, 3))
    blk_update, blk_moment = lion_step(clipped, blk_plain)
    return (to_owner(emb_update), to_owner(emb_moment), jnp.transpose(blk_update, (0, 2, 1, 3)), jnp.transpose(blk_moment, (0, 2, 1, 3)))
```

```python
import functools

import jax
import jax.numpy as jnp
from jax import lax
from jax.experimental import pallas as pl
from jax.experimental.pallas import tpu as pltpu
from jax.sharding import Mesh
from jax.sharding import PartitionSpec as P


DP = ("dp_0", "dp_1")
MP = ("mp_0", "mp_1", "mp_2")
DP_MP = DP + MP


beta_first = 0.9
beta_second = 0.99
temper = 0.05
epsilon = 1e-06

VMEM_BYTES = 67_043_328
LION_BYTES = 24 * 1024 * 1024
F32 = jnp.float32
BF16 = jnp.bfloat16
ANY = pl.BlockSpec(memory_space=pltpu.HBM)
VMEM = pl.BlockSpec(memory_space=pltpu.VMEM)
SMEM = pl.BlockSpec(memory_space=pltpu.SMEM)

EMB_ROWS = 2080
BLK_ROWS = 520
SUM_ROW = 512
SUM_LANE = 96


EMB_STEPS = [(0, 1), (1, 0), (1, 1), (2, 0), (2, 1), (3, 0), (3, 1), (0, 0)]


def emb_peer(a, b, step, sign):
    return ((a + sign * step[0] + 4) % 4) * 2 + (b ^ step[1])


def lanes(shape):
    return lax.broadcasted_iota(jnp.int32, shape, len(shape) - 1)


def split_three(value):
    high = value.astype(BF16).astype(F32)
    middle = (value - high).astype(BF16).astype(F32)
    low = (value - high - middle).astype(BF16).astype(F32)
    return high, middle, low


def fold8(x):
    return jnp.sum(x.reshape(x.shape[0] // 8, 8, x.shape[1]), axis=0)


def emb_peers(sign):
    a, b = (lax.axis_index(name) for name in DP)
    return [emb_peer(a, b, step, sign) for step in EMB_STEPS]


def blk_pack_kernel(groups, label_ref, grad, emb, *rest):
    dp_index = lax.axis_index("dp_0") * 2 + lax.axis_index("dp_1")
    mp_index = lax.axis_index("mp_0") * 4 + lax.axis_index("mp_1") * 2 + lax.axis_index("mp_2")
    out, stage, xb, xe, bsem, esem, osem = rest
    matrices, block_rows, block_cols = xb.shape
    count = stage.shape[0]
    owner_rows = block_rows // count
    half = block_rows // 2
    step = 64
    steps = xe.shape[0] // step
    for m in range(matrices):
        pltpu.make_async_copy(grad.at[m], xb.at[m], bsem.at[m]).start()
    for g in range(steps):
        pltpu.make_async_copy(
            emb.at[pl.ds(g * step, step)], xe.at[pl.ds(g * step, step)], esem.at[g]
        ).start()
    full = block_cols // 128
    for m in range(matrices):
        pltpu.make_async_copy(grad.at[m], xb.at[m], bsem.at[m]).wait()
    block_sums = []
    for m in range(matrices):
        for h in range(2):
            x = xb[m, h * half : (h + 1) * half, :].astype(F32)
            block_sums.append(jnp.sum(fold8(x * x)))
    for j in range(count):
        x = jnp.concatenate(
            [xb[m, j * owner_rows : (j + 1) * owner_rows, :].astype(F32) for m in range(matrices)],
            axis=0,
        )
        rows = x.shape[0]
        for t in range(full):
            stage[j, t * rows : (t + 1) * rows, :] = x[:, t * 128 : (t + 1) * 128].astype(BF16)
        tail = x[:, full * 128 :]
        for q in range(4):
            part = tail[q * 16 : min(q * 16 + 16, rows), :].astype(BF16)
            base = rows * full
            stage[j, base : base + part.shape[0], q * 32 : (q + 1) * 32] = part
    acc = jnp.zeros((8, 512), F32)
    tail_acc = jnp.zeros((8, xe.shape[1] % 512), F32)
    for g in range(steps):
        pltpu.make_async_copy(
            emb.at[pl.ds(g * step, step)], xe.at[pl.ds(g * step, step)], esem.at[g]
        ).wait()
        for c in range(xe.shape[1] // 512):
            x = xe[g * step : (g + 1) * step, c * 512 : (c + 1) * 512].astype(F32)
            acc = acc + fold8(x * x)
        x = xe[g * step : (g + 1) * step, xe.shape[1] // 512 * 512 :].astype(F32)
        tail_acc = tail_acc + fold8(x * x)
    emb_sum = jnp.sum(acc) + jnp.sum(tail_acc)
    lane = lanes((8, 128))
    sums = jnp.zeros((8, 128), F32)
    for g in range(groups):
        total = emb_sum if g == 0 else jnp.float32(0)
        for i, s in enumerate(block_sums):
            label = label_ref[i // 2, dp_index * 2 + i % 2, mp_index]
            total = total + jnp.where(label == g, s, jnp.float32(0))
        for p, piece in enumerate(split_three(jnp.full((8, 128), total, F32))):
            sums = jnp.where(lane == SUM_LANE + 3 * g + p, piece, sums)
    for j in range(count):
        old = stage[j, SUM_ROW:, :].astype(F32)
        stage[j, SUM_ROW:, :] = jnp.where(lane < SUM_LANE, old, sums).astype(BF16)
    copy = pltpu.make_async_copy(stage, out, osem.at[0])
    copy.start()
    copy.wait()


def emb_pack_kernel(emb, *rest):
    dest = emb_peers(1)
    outs, (stage, xe, esem, osem) = rest[:8], rest[8:]
    features, tile_rows = xe.shape
    count = stage.shape[0]
    own_rows = tile_rows // count
    step = 64
    steps = features // step
    full = own_rows // 128
    rest_lanes = own_rows - full * 128 - 64
    for g in range(steps):
        pltpu.make_async_copy(
            emb.at[pl.ds(g * step, step)], xe.at[pl.ds(g * step, step)], esem.at[g]
        ).start()
    lane = lanes((step, 128))
    low = lanes((step // 2, 128)) < 64
    for g in range(steps):
        pltpu.make_async_copy(
            emb.at[pl.ds(g * step, step)], xe.at[pl.ds(g * step, step)], esem.at[g]
        ).wait()

        def tile(i):
            x = xe[g * step : (g + 1) * step, i * 128 : min(i * 128 + 128, tile_rows)].astype(F32)
            if x.shape[1] < 128:
                x = jnp.concatenate([x, jnp.zeros((step, 128 - x.shape[1]), F32)], axis=1)
            return x

        for d in range(count):
            q, r = divmod(d * own_rows, 128)
            need = -(-(r + own_rows) // 128)
            turned = [pltpu.roll(tile(q + i), (128 - r) % 128, 1) if r else tile(q + i) for i in range(need)]
            for t in range(full + 1):
                x = turned[t]
                if r and t + 1 < need:
                    x = jnp.where(lane < 128 - r, x, turned[t + 1])
                if t < full:
                    stage[d, t * features + g * step : t * features + (g + 1) * step, :] = x.astype(BF16)
            half = step // 2
            both = jnp.where(low, x[:half], pltpu.roll(x[half:], 64, 1))
            base = full * features
            stage[d, base + g * half : base + (g + 1) * half, :] = both.astype(BF16)
            base = base + features // 2
            moved = pltpu.roll(x, (rest_lanes * g + 64) % 128, 1)
            if g:
                old = stage[d, base:, :].astype(F32)
                moved = jnp.where(lane < rest_lanes * g, old, moved)
            stage[d, base:, :] = moved.astype(BF16)
    copies = [
        pltpu.make_async_copy(stage.at[dest[k]], out, osem.at[k]) for k, out in enumerate(outs)
    ]
    for c in copies:
        c.start()
    for c in copies:
        c.wait()


def step_of(grad, factor, moment):
    clipped = grad * factor
    update = jnp.tanh((beta_first * moment + (1.0 - beta_first) * clipped) / temper)
    return update.astype(BF16), (beta_second * moment + (1.0 - beta_second) * clipped).astype(BF16)


def blk_lion_kernel(factor_ref, *rest):
    stage, mv, update, moment, wide, uv, nv, osem = rest
    count, mom = stage.shape[0], mv
    matrices, owner_rows, _, block_cols = mom.shape
    rows = matrices * owner_rows
    full = block_cols // 128
    for s in range(count):
        for m in range(matrices):
            f = factor_ref[m, s]
            for t in range(full):
                x = stage[s, t * rows + m * owner_rows : t * rows + (m + 1) * owner_rows, :].astype(F32)
                wide[t, pl.ds(m * owner_rows * count + s, owner_rows, stride=count), :] = x * f
        tail = []
        for q in range(4):
            n = min(16, rows - q * 16)
            x = stage[s, rows * full : rows * full + 16, :].astype(F32)
            tail.append((pltpu.roll(x, 128 - 32 * q, 1) if q else x)[:n])
        tail = jnp.concatenate(tail, axis=0)
        for m in range(matrices):
            f = factor_ref[m, s]
            wide[full, pl.ds(m * owner_rows * count + s, owner_rows, stride=count), :] = (
                tail[m * owner_rows : (m + 1) * owner_rows] * f
            )
    for m in range(matrices):
        for r in range(owner_rows):
            base = (m * owner_rows + r) * count
            for t in range(full + 1):
                cols = slice(t * 128, min(t * 128 + 128, block_cols))
                grad = wide[t, base : base + count, : cols.stop - cols.start]
                up, new = step_of(grad, 1.0, mv[m, r, :, cols].astype(F32))
                uv[m, r, :, cols] = up
                nv[m, r, :, cols] = new
        pltpu.make_async_copy(uv.at[m], update.at[m], osem.at[m]).start()
        pltpu.make_async_copy(nv.at[m], moment.at[m], osem.at[2 + m]).start()
    for m in range(matrices):
        pltpu.make_async_copy(uv.at[m], update.at[m], osem.at[m]).wait()
        pltpu.make_async_copy(nv.at[m], moment.at[m], osem.at[2 + m]).wait()


def emb_lion_kernel(which, chained, factor_ref, *rest):
    n = len(which)
    source = [emb_peers(-1)[i] for i in which]
    parts, rest = rest[:n], rest[n:]
    mom, rest = rest[0], rest[1:]
    if chained:
        rest = rest[2:]
    update, moment, uv, nv, usem, nsem = rest
    _, features, own_rows = mom.shape
    step = 64
    full = own_rows // 128
    rest_lanes = own_rows - full * 128 - 64
    f = factor_ref[0]
    low = lanes((step, 128)) < 64
    for k in range(n):
        for g in range(features // step):
            rows = slice(g * step, (g + 1) * step)
            for t in range(full + 1):
                cols = slice(t * 128, min(t * 128 + 128, own_rows))
                if t < full:
                    x = parts[k][t * features + g * step : t * features + (g + 1) * step, :].astype(F32)
                else:
                    half = step // 2
                    base = full * features
                    both = parts[k][base + g * half : base + (g + 1) * half, :].astype(F32)
                    left = jnp.concatenate([both, pltpu.roll(both, 64, 1)], axis=0)
                    base = base + features // 2
                    right = pltpu.roll(parts[k][base:, :].astype(F32), (64 - rest_lanes * g) % 128, 1)
                    x = jnp.where(low, left, right)[:, : own_rows - full * 128]
                up, new = step_of(x, f, mom[source[k], rows, cols].astype(F32))
                uv[k, rows, cols] = up
                nv[k, rows, cols] = new
        pltpu.make_async_copy(uv.at[k], update.at[source[k]], usem.at[k]).start()
        pltpu.make_async_copy(nv.at[k], moment.at[source[k]], nsem.at[k]).start()
    for k in range(n):
        pltpu.make_async_copy(uv.at[k], update.at[source[k]], usem.at[k]).wait()
        pltpu.make_async_copy(nv.at[k], moment.at[source[k]], nsem.at[k]).wait()


def emb_lion(parts, which, factor, mom, prior):
    n = len(which)
    shape = jax.ShapeDtypeStruct(mom.shape, BF16)
    buffers = [pltpu.VMEM((n,) + mom.shape[1:], BF16)] * 2
    extra = () if prior is None else prior
    first = 1 + n + 1
    return pl.pallas_call(
        functools.partial(emb_lion_kernel, tuple(which), prior is not None),
        out_shape=(shape, shape),
        in_specs=[SMEM] + [VMEM] * (n + 1) + [ANY] * len(extra),
        out_specs=(ANY, ANY),
        scratch_shapes=buffers + [pltpu.SemaphoreType.DMA((n,))] * 2,
        input_output_aliases={first: 0, first + 1: 1} if extra else {},
        compiler_params=pltpu.CompilerParams(vmem_limit_bytes=LION_BYTES),
        cost_estimate=pl.CostEstimate(flops=n * 3_000_000, bytes_accessed=n * 2_300_000, transcendentals=0),
    )(factor, *[parts[i] for i in which], mom, *extra)


def emb_send(value, step):
    pairs = [(a * 2 + b, emb_peer(a, b, step, 1)) for a in range(4) for b in range(2)]
    return lax.ppermute(value, DP, pairs)


def on_device(emb_grad, emb_mom, blk_grad, blk_mom, tile_group, clip_rms):
    dp_count = lax.axis_size(DP)
    mp_count = lax.axis_size(MP)
    a, b = lax.axis_index("dp_0"), lax.axis_index("dp_1")
    z, x, c = (lax.axis_index(name) for name in MP)
    dp_index = a * 2 + b
    mp_index = z * 4 + x * 2 + c
    groups = clip_rms.shape[0]
    tile_rows, tile_cols = emb_grad.shape
    own_rows = emb_mom.shape[3]
    matrices, block_rows, block_cols = blk_grad.shape
    owner_rows = blk_mom.shape[2]
    row_blocks = tile_group.shape[1] // dp_count
    block_height = block_rows // row_blocks
    emb_t = emb_grad.T
    packed = pl.pallas_call(
        functools.partial(blk_pack_kernel, groups),
        out_shape=jax.ShapeDtypeStruct((mp_count, BLK_ROWS, 128), BF16),
        in_specs=[SMEM, ANY, ANY],
        out_specs=ANY,
        scratch_shapes=[
            pltpu.VMEM((16, BLK_ROWS, 128), BF16),
            pltpu.VMEM(blk_grad.shape, BF16),
            pltpu.VMEM(emb_t.shape, BF16),
            pltpu.SemaphoreType.DMA((2,)),
            pltpu.SemaphoreType.DMA((7,)),
            pltpu.SemaphoreType.DMA((1,)),
        ],
        compiler_params=pltpu.CompilerParams(vmem_limit_bytes=VMEM_BYTES),
        cost_estimate=pl.CostEstimate(flops=10_000_000, bytes_accessed=9_000_000, transcendentals=0),
        name="blk_pack",
    )(tile_group, blk_grad, emb_t)
    blk_parts = lax.all_to_all(packed, MP, split_axis=0, concat_axis=0, tiled=True)

    emb_payload = jax.ShapeDtypeStruct((EMB_ROWS, 128), BF16)
    emb_packed = pl.pallas_call(
        emb_pack_kernel,
        out_shape=(emb_payload,) * 8,
        in_specs=[ANY],
        out_specs=(ANY,) * 8,
        scratch_shapes=[
            pltpu.VMEM((8, EMB_ROWS, 128), BF16),
            pltpu.VMEM(emb_t.shape, BF16),
            pltpu.SemaphoreType.DMA((7,)),
            pltpu.SemaphoreType.DMA((8,)),
        ],
        compiler_params=pltpu.CompilerParams(vmem_limit_bytes=VMEM_BYTES),
        cost_estimate=pl.CostEstimate(flops=10_000_000, bytes_accessed=9_000_000, transcendentals=0),
        name="emb_pack",
    )(emb_t)
    emb_parts = [emb_send(v, s) for v, s in zip(emb_packed[:7], EMB_STEPS)] + [emb_packed[7]]

    pieces = jnp.sum(blk_parts[:, SUM_ROW, SUM_LANE : SUM_LANE + 3 * groups].astype(F32), axis=0)
    pieces = sum(emb_send(pieces, s) for s in EMB_STEPS[:7]) + pieces
    totals = jnp.sum(pieces.reshape(groups, 3), axis=1)

    labels = jnp.arange(groups, dtype=jnp.int32)
    first = (labels == 0).astype(F32)
    onehot = (tile_group[..., None] == labels).astype(F32)
    counts = jnp.sum(onehot, axis=(0, 1, 2)) * float(block_height * block_cols) + first * float(
        tile_rows * mp_count * tile_cols * dp_count
    )
    root_mean = jnp.sqrt(totals / jnp.maximum(counts, 1.0))
    factor = jnp.minimum(1.0, clip_rms / (root_mean + epsilon))
    owner_block = dp_index * row_blocks + mp_index * owner_rows // block_height
    owner_ids = lax.dynamic_index_in_dim(onehot, owner_block, axis=1, keepdims=False)
    owner_factor = jnp.sum(owner_ids * factor, axis=-1)

    mom_t = jnp.transpose(blk_mom, (0, 2, 1, 3))
    shape = jax.ShapeDtypeStruct(mom_t.shape, BF16)
    blk_update, blk_moment = pl.pallas_call(
        blk_lion_kernel,
        out_shape=(shape, shape),
        in_specs=[SMEM, VMEM, VMEM],
        out_specs=(ANY, ANY),
        scratch_shapes=[
            pltpu.VMEM((block_cols // 128 + 1, matrices * owner_rows * 16, 128), F32),
            pltpu.VMEM(mom_t.shape, BF16),
            pltpu.VMEM(mom_t.shape, BF16),
            pltpu.SemaphoreType.DMA((4,)),
        ],
        compiler_params=pltpu.CompilerParams(vmem_limit_bytes=LION_BYTES),
        cost_estimate=pl.CostEstimate(flops=10_000_000, bytes_accessed=9_000_000, transcendentals=0),
        name="blk_lion",
    )(owner_factor, blk_parts, mom_t)

    emb_mom_t = jnp.transpose(emb_mom.reshape(dp_count, own_rows, tile_cols), (0, 2, 1))
    early = [7, 0, 1, 3, 5, 2]
    late = [4, 6]
    outs = None
    for which in (early, late):
        outs = emb_lion(
            emb_parts,
            which,
            factor[:1],
            emb_mom_t,
            outs,
        )
    emb_update, emb_moment = (jnp.transpose(v, (0, 2, 1)).reshape(emb_mom.shape) for v in outs)
    return (
        emb_update,
        emb_moment,
        jnp.transpose(blk_update, (0, 2, 1, 3)),
        jnp.transpose(blk_moment, (0, 2, 1, 3)),
    )


def solution(mesh):
    torus = Mesh(mesh.devices.reshape(4, 2, 4, 2, 2), DP_MP)
    return jax.shard_map(
        on_device,
        mesh=torus,
        in_specs=(
            P(MP, DP),
            P(MP, None, DP, None, None),
            P(None, DP, MP),
            P(None, None, DP_MP, None),
            P(),
            P(),
        ),
        out_specs=(
            P(MP, None, DP, None, None),
            P(MP, None, DP, None, None),
            P(None, None, DP_MP, None),
            P(None, None, DP_MP, None),
        ),
        check_vma=False,
    )
```

```python
import functools

import jax
import jax.numpy as jnp
from jax import lax
from jax.experimental import pallas as pl
from jax.experimental.pallas import tpu as pltpu
from jax.sharding import Mesh
from jax.sharding import PartitionSpec as P


DP = ("dp_0", "dp_1")
MP = ("mp_0", "mp_1", "mp_2")
DP_MP = DP + MP


beta_first = 0.9
beta_second = 0.99
temper = 0.05
epsilon = 1e-06

VMEM_BYTES = 67_043_328
F32 = jnp.float32
BF16 = jnp.bfloat16
ANY = pl.BlockSpec(memory_space=pltpu.HBM)
VMEM = pl.BlockSpec(memory_space=pltpu.VMEM)
SMEM = pl.BlockSpec(memory_space=pltpu.SMEM)

EMB_ROWS = 2080
BLK_ROWS = 520
SUM_ROW = 512
SUM_LANE = 96


EMB_STEPS = [(0, 1), (1, 0), (1, 1), (2, 0), (2, 1), (3, 0), (3, 1), (0, 0)]


def emb_peer(a, b, step, sign):
    return ((a + sign * step[0] + 4) % 4) * 2 + (b ^ step[1])


def lanes(shape):
    return lax.broadcasted_iota(jnp.int32, shape, len(shape) - 1)


def split_three(value):
    high = value.astype(BF16).astype(F32)
    middle = (value - high).astype(BF16).astype(F32)
    low = (value - high - middle).astype(BF16).astype(F32)
    return high, middle, low


def fold8(x):
    return jnp.sum(x.reshape(x.shape[0] // 8, 8, x.shape[1]), axis=0)


def emb_peers(sign):
    a, b = (lax.axis_index(name) for name in DP)
    return [emb_peer(a, b, step, sign) for step in EMB_STEPS]


def blk_pack_kernel(groups, label_ref, grad, emb, *rest):
    dp_index = lax.axis_index("dp_0") * 2 + lax.axis_index("dp_1")
    mp_index = lax.axis_index("mp_0") * 4 + lax.axis_index("mp_1") * 2 + lax.axis_index("mp_2")
    out, stage, ending, xb, xe, bsem, esem, osem = rest
    matrices, block_rows, block_cols = xb.shape
    count = stage.shape[0]
    owner_rows = block_rows // count
    half = block_rows // 2
    step = 64
    steps = xe.shape[0] // step
    for m in range(matrices):
        pltpu.make_async_copy(grad.at[m], xb.at[m], bsem.at[m]).start()
    for g in range(steps):
        pltpu.make_async_copy(
            emb.at[pl.ds(g * step, step)], xe.at[pl.ds(g * step, step)], esem.at[g]
        ).start()
    full = block_cols // 128
    for m in range(matrices):
        pltpu.make_async_copy(grad.at[m], xb.at[m], bsem.at[m]).wait()
    block_sums = []
    for m in range(matrices):
        for h in range(2):
            x = xb[m, h * half : (h + 1) * half, :].astype(F32)
            block_sums.append(jnp.sum(fold8(x * x)))
    for j in range(count):
        x = jnp.concatenate(
            [xb[m, j * owner_rows : (j + 1) * owner_rows, :].astype(F32) for m in range(matrices)],
            axis=0,
        )
        rows = x.shape[0]
        for t in range(full):
            stage[j, t * rows : (t + 1) * rows, :] = x[:, t * 128 : (t + 1) * 128].astype(BF16)
        tail = x[:, full * 128 :]
        for q in range(4):
            base = rows * full
            stage[j, base : base + 8, q * 32 : (q + 1) * 32] = tail[q * 16 : q * 16 + 8, :].astype(BF16)
            if q < 3:
                ending[j, :, q * 32 : (q + 1) * 32] = tail[q * 16 + 8 : q * 16 + 16, :].astype(BF16)
    main = pltpu.make_async_copy(stage, out.at[:, pl.ds(0, SUM_ROW)], osem.at[0])
    main.start()
    acc = jnp.zeros((8, 512), F32)
    tail_acc = jnp.zeros((8, xe.shape[1] % 512), F32)
    for g in range(steps):
        pltpu.make_async_copy(
            emb.at[pl.ds(g * step, step)], xe.at[pl.ds(g * step, step)], esem.at[g]
        ).wait()
        for c in range(xe.shape[1] // 512):
            x = xe[g * step : (g + 1) * step, c * 512 : (c + 1) * 512].astype(F32)
            acc = acc + fold8(x * x)
        x = xe[g * step : (g + 1) * step, xe.shape[1] // 512 * 512 :].astype(F32)
        tail_acc = tail_acc + fold8(x * x)
    emb_sum = jnp.sum(acc) + jnp.sum(tail_acc)
    lane = lanes((8, 128))
    sums = jnp.zeros((8, 128), F32)
    for g in range(groups):
        total = emb_sum if g == 0 else jnp.float32(0)
        for i, s in enumerate(block_sums):
            label = label_ref[i // 2, dp_index * 2 + i % 2, mp_index]
            total = total + jnp.where(label == g, s, jnp.float32(0))
        for p, piece in enumerate(split_three(jnp.full((8, 128), total, F32))):
            sums = jnp.where(lane == SUM_LANE + 3 * g + p, piece, sums)
    for j in range(count):
        ending[j] = jnp.where(lane < SUM_LANE, ending[j].astype(F32), sums).astype(BF16)
    last = pltpu.make_async_copy(ending, out.at[:, pl.ds(SUM_ROW, 8)], osem.at[1])
    last.start()
    main.wait()
    last.wait()


def emb_pack_rows(tile, write, features, own_rows, d, g, step):
    full = own_rows // 128
    rest_lanes = own_rows - full * 128 - 64
    lane = lanes((step, 128))
    low = lanes((step // 2, 128)) < 64
    q, r = divmod(d * own_rows, 128)
    need = -(-(r + own_rows) // 128)
    turned = [pltpu.roll(tile(q + i), 128 - r, 1) if r else tile(q + i) for i in range(need)]
    for t in range(full + 1):
        x = turned[t]
        if r and t + 1 < need:
            x = jnp.where(lane < 128 - r, x, turned[t + 1])
        if t < full:
            write[t * features + g * step : t * features + (g + 1) * step, :] = x.astype(BF16)
    half = step // 2
    both = jnp.where(low, x[:half], pltpu.roll(x[half:], 64, 1))
    base = full * features
    write[base + g * half : base + (g + 1) * half, :] = both.astype(BF16)
    base = base + features // 2
    moved = pltpu.roll(x, (rest_lanes * g + 64) % 128, 1)
    if g:
        old = write[base:, :].astype(F32)
        moved = jnp.where(lane < rest_lanes * g, old, moved)
    write[base:, :] = moved.astype(BF16)


def tile_of(ref, g, step, i, first, limit):
    start = (i - first) * 128
    x = ref[g * step : (g + 1) * step, start : min(start + 128, limit)].astype(F32)
    if x.shape[1] < 128:
        x = jnp.concatenate([x, jnp.zeros((step, 128 - x.shape[1]), F32)], axis=1)
    return x


def emb_first_kernel(own_rows, emb, *rest):
    n = len(FIRST)
    outs, (stage, xe, esem, osem) = rest[:n], rest[n:]
    dest = emb_peers(1)
    features, tile_rows = emb.shape
    step = 64
    copies = [
        pltpu.make_async_copy(emb.at[pl.ds(g * step, step)], xe.at[pl.ds(g * step, step)], esem.at[g])
        for g in range(features // step)
    ]
    for c in copies:
        c.start()
    for g in range(features // step):
        copies[g].wait()
        tile = functools.partial(tile_of, xe, g, step, first=0, limit=tile_rows)
        for d in range(tile_rows // own_rows):
            for k, i in enumerate(FIRST):

                @pl.when(dest[i] == d)
                def _():
                    emb_pack_rows(tile, stage.at[k], features, own_rows, d, g, step)

    copies = [pltpu.make_async_copy(stage.at[k], out, osem.at[k]) for k, out in enumerate(outs)]
    for c in copies:
        c.start()
    for c in copies:
        c.wait()


def emb_pack_kernel(emb, *rest):
    outs, (stage, xe, esem, osem) = rest[: len(REST)], rest[len(REST) :]
    dest = emb_peers(1)
    features, tile_rows = xe.shape
    count = stage.shape[0]
    step = 64
    copies = [
        pltpu.make_async_copy(emb.at[pl.ds(g * step, step)], xe.at[pl.ds(g * step, step)], esem.at[g])
        for g in range(features // step)
    ]
    for c in copies:
        c.start()
    for g in range(features // step):
        copies[g].wait()
        tile = functools.partial(tile_of, xe, g, step, first=0, limit=tile_rows)
        for d in range(count):
            emb_pack_rows(tile, stage.at[d], features, tile_rows // count, d, g, step)
    copies = [
        pltpu.make_async_copy(stage.at[dest[i]], out, osem.at[k]) for k, (i, out) in enumerate(zip(REST, outs))
    ]
    for c in copies:
        c.start()
    for c in copies:
        c.wait()


def step_of(grad, factor, moment):
    clipped = grad * factor
    update = jnp.tanh((beta_first * moment + (1.0 - beta_first) * clipped) / temper)
    return update.astype(BF16), (beta_second * moment + (1.0 - beta_second) * clipped).astype(BF16)


def mix_kernel(parts, out, stage, wide, mixed, psem, osem):
    count, _, _ = stage.shape
    matrices, owner_rows, _, block_cols = mixed.shape
    rows = matrices * owner_rows
    full = block_cols // 128
    copy = pltpu.make_async_copy(parts, stage, psem)
    copy.start()
    copy.wait()
    for s in range(count):
        for m in range(matrices):
            place = pl.ds(m * owner_rows * count + s, owner_rows, stride=count)
            for t in range(full):
                x = stage[s, t * rows + m * owner_rows : t * rows + (m + 1) * owner_rows, :]
                wide[t, place, :] = x.astype(F32)
        tail = []
        for q in range(4):
            n = min(16, rows - q * 16)
            x = stage[s, rows * full : rows * full + 16, :].astype(F32)
            tail.append((pltpu.roll(x, 128 - 32 * q, 1) if q else x)[:n])
        tail = jnp.concatenate(tail, axis=0)
        for m in range(matrices):
            place = pl.ds(m * owner_rows * count + s, owner_rows, stride=count)
            wide[full, place, :] = tail[m * owner_rows : (m + 1) * owner_rows]
    for m in range(matrices):
        for r in range(owner_rows):
            base = (m * owner_rows + r) * count
            for t in range(full + 1):
                cols = slice(t * 128, min(t * 128 + 128, block_cols))
                x = wide[t, base : base + count, : cols.stop - cols.start]
                mixed[m, r, :, cols] = x.astype(BF16)
    copy = pltpu.make_async_copy(mixed, out, osem)
    copy.start()
    copy.wait()


def emb_lion_chunk(part, mom, up, new, f):
    features, own_rows = up.shape
    step = 64
    f = jnp.concatenate([f] * (step // 8), axis=0)
    full = own_rows // 128
    rest_lanes = own_rows - full * 128 - 64
    low = lanes((step, 128)) < 64
    for g in range(features // step):
        rows = slice(g * step, (g + 1) * step)
        for t in range(full + 1):
            cols = slice(t * 128, min(t * 128 + 128, own_rows))
            if t < full:
                x = part[t * features + g * step : t * features + (g + 1) * step, :].astype(F32)
            else:
                half = step // 2
                base = full * features
                both = part[base + g * half : base + (g + 1) * half, :].astype(F32)
                left = jnp.concatenate([both, pltpu.roll(both, 64, 1)], axis=0)
                base = base + features // 2
                right = pltpu.roll(part[base:, :].astype(F32), (64 - rest_lanes * g) % 128, 1)
                x = jnp.where(low, left, right)[:, : own_rows - full * 128]
            up[rows, cols], new[rows, cols] = step_of(
                x, f[:, : cols.stop - cols.start], mom[rows, cols].astype(F32)
            )


def group_factor(g, shares_ref, counts_ref, clip_ref):
    total = jnp.float32(0)
    for p in range(3):
        piece = shares_ref[0, 3 * g + p]
        for d in range(1, shares_ref.shape[0]):
            piece = piece + shares_ref[d, 3 * g + p]
        total = total + piece
    total, count, clip = (jnp.full((8, 128), v, F32) for v in (total, counts_ref[g], clip_ref[g]))
    root_mean = jnp.sqrt(total / jnp.maximum(count, 1.0))
    return jnp.minimum(1.0, clip / (root_mean + epsilon))


def lion_kernel(which, shares_ref, counts_ref, clip_ref, label_ref, mixed, blk_mom, emb_mom, *rest):
    n = len(which)
    parts, rest = rest[:n], rest[n:]
    emb_up, emb_new, blk_up, blk_new, gv, bv, pv, ev, eu, en, bu, bn, isem, osem = rest
    source = [emb_peers(-1)[i] for i in which]
    matrices, owner_rows, count, block_cols = blk_mom.shape
    copy = pltpu.make_async_copy
    loads, stores = [], []
    for m in range(matrices):
        loads.append([(mixed.at[m], gv.at[m]), (blk_mom.at[m], bv.at[m])])
        stores.append([(bu.at[m], blk_up.at[m]), (bn.at[m], blk_new.at[m])])
    for k in range(n):
        loads.append([(parts[k], pv.at[k]), (emb_mom.at[source[k]], ev.at[k])])
        stores.append([(eu.at[k], emb_up.at[source[k]]), (en.at[k], emb_new.at[source[k]])])
    loads = [[copy(*c, isem.at[2 * i + j]) for j, c in enumerate(cs)] for i, cs in enumerate(loads)]
    stores = [[copy(*c, osem.at[2 * i + j]) for j, c in enumerate(cs)] for i, cs in enumerate(stores)]
    ahead = 3
    for cs in loads[:ahead]:
        for c in cs:
            c.start()
    factors = [group_factor(g, shares_ref, counts_ref, clip_ref) for g in range(clip_ref.shape[0])]
    row_blocks = label_ref.shape[1]
    dp_index = lax.axis_index("dp_0") * 2 + lax.axis_index("dp_1")
    mp_index = lax.axis_index("mp_0") * 4 + lax.axis_index("mp_1") * 2 + lax.axis_index("mp_2")
    per_dp = row_blocks // 8
    owner_block = dp_index * per_dp + mp_index * per_dp // count
    sublane = lax.broadcasted_iota(jnp.int32, (count, 128), 0)
    for i, cs in enumerate(loads):
        for c in cs:
            c.wait()
        for c in loads[i + ahead] if i + ahead < len(loads) else []:
            c.start()
        if i < matrices:
            f = jnp.zeros((count, 128), F32)
            for s in range(count):
                label = label_ref[i, owner_block, s]
                own = factors[0]
                for g in range(1, len(factors)):
                    own = jnp.where(label == g, factors[g], own)
                f = jnp.where(sublane == s, jnp.concatenate([own] * (count // 8), axis=0), f)
            for r in range(owner_rows):
                for t in range(block_cols // 128 + 1):
                    cols = slice(t * 128, min(t * 128 + 128, block_cols))
                    bu[i, r, :, cols], bn[i, r, :, cols] = step_of(
                        gv[i, r, :, cols].astype(F32),
                        f[:, : cols.stop - cols.start],
                        bv[i, r, :, cols].astype(F32),
                    )
        else:
            k = i - matrices
            emb_lion_chunk(pv.at[k], ev.at[k], eu.at[k], en.at[k], factors[0])
        for c in stores[i]:
            c.start()
    for cs in stores:
        for c in cs:
            c.wait()


def last_kernel(which, shares_ref, counts_ref, clip_ref, emb_mom, *rest):
    n = len(which)
    parts, (_, _, emb_up, emb_new, pv, ev, eu, en, isem, osem) = rest[:n], rest[n:]
    source = [emb_peers(-1)[i] for i in which]
    copy = pltpu.make_async_copy
    loads, stores = [], []
    for k in range(n):
        loads += [copy(parts[k], pv.at[k], isem.at[2 * k]), copy(emb_mom.at[source[k]], ev.at[k], isem.at[2 * k + 1])]
        stores += [
            copy(eu.at[k], emb_up.at[source[k]], osem.at[2 * k]),
            copy(en.at[k], emb_new.at[source[k]], osem.at[2 * k + 1]),
        ]
    for c in loads:
        c.start()
    factor = group_factor(0, shares_ref, counts_ref, clip_ref)
    for k in range(n):
        for c in loads[2 * k : 2 * k + 2]:
            c.wait()
        emb_lion_chunk(pv.at[k], ev.at[k], eu.at[k], en.at[k], factor)
        for c in stores[2 * k : 2 * k + 2]:
            c.start()
    for c in stores:
        c.wait()


def emb_send(value, step):
    pairs = [(a * 2 + b, emb_peer(a, b, step, 1)) for a in range(4) for b in range(2)]
    return lax.ppermute(value, DP, pairs)


def on_device(emb_grad, emb_mom, blk_grad, blk_mom, tile_group, clip_rms):
    dp_count = lax.axis_size(DP)
    mp_count = lax.axis_size(MP)
    z, x, c = (lax.axis_index(name) for name in MP)
    groups = clip_rms.shape[0]
    tile_rows, tile_cols = emb_grad.shape
    own_rows = emb_mom.shape[3]
    matrices, block_rows, block_cols = blk_grad.shape
    owner_rows = blk_mom.shape[2]
    row_blocks = tile_group.shape[1] // dp_count
    block_height = block_rows // row_blocks
    emb_t = emb_grad.T
    emb_payload = jax.ShapeDtypeStruct((EMB_ROWS, 128), BF16)
    emb_first = pl.pallas_call(
        functools.partial(emb_first_kernel, own_rows),
        out_shape=(emb_payload,) * len(FIRST),
        in_specs=[ANY],
        out_specs=(ANY,) * len(FIRST),
        scratch_shapes=[
            pltpu.VMEM((len(FIRST), EMB_ROWS, 128), BF16),
            pltpu.VMEM(emb_t.shape, BF16),
            pltpu.SemaphoreType.DMA((7,)),
            pltpu.SemaphoreType.DMA((len(FIRST),)),
        ],
        compiler_params=pltpu.CompilerParams(vmem_limit_bytes=VMEM_BYTES),
        cost_estimate=pl.CostEstimate(flops=2_000_000, bytes_accessed=1_200_000, transcendentals=0),
        name="emb_first",
    )(emb_t)
    packed = pl.pallas_call(
        functools.partial(blk_pack_kernel, groups),
        out_shape=jax.ShapeDtypeStruct((mp_count, BLK_ROWS, 128), BF16),
        in_specs=[SMEM, ANY, ANY],
        out_specs=ANY,
        scratch_shapes=[
            pltpu.VMEM((16, SUM_ROW, 128), BF16),
            pltpu.VMEM((16, BLK_ROWS - SUM_ROW, 128), BF16),
            pltpu.VMEM(blk_grad.shape, BF16),
            pltpu.VMEM(emb_t.shape, BF16),
            pltpu.SemaphoreType.DMA((2,)),
            pltpu.SemaphoreType.DMA((7,)),
            pltpu.SemaphoreType.DMA((2,)),
        ],
        compiler_params=pltpu.CompilerParams(vmem_limit_bytes=VMEM_BYTES),
        cost_estimate=pl.CostEstimate(flops=10_000_000, bytes_accessed=9_000_000, transcendentals=0),
        name="blk_pack",
    )(tile_group, blk_grad, emb_t)
    blk_parts = lax.all_to_all(packed, MP, split_axis=0, concat_axis=0, tiled=True)

    emb_packed = pl.pallas_call(
        emb_pack_kernel,
        out_shape=(emb_payload,) * len(REST),
        in_specs=[ANY],
        out_specs=(ANY,) * len(REST),
        scratch_shapes=[
            pltpu.VMEM((8, EMB_ROWS, 128), BF16),
            pltpu.VMEM(emb_t.shape, BF16),
            pltpu.SemaphoreType.DMA((7,)),
            pltpu.SemaphoreType.DMA((7,)),
        ],
        compiler_params=pltpu.CompilerParams(vmem_limit_bytes=VMEM_BYTES),
        cost_estimate=pl.CostEstimate(flops=10_000_000, bytes_accessed=9_000_000, transcendentals=0),
        name="emb_pack",
    )(emb_t)
    payloads = dict(zip(FIRST + REST, (*emb_first, *emb_packed)))
    emb_parts = [emb_send(payloads[i], EMB_STEPS[i]) for i in range(7)] + [payloads[7]]

    pieces = jnp.sum(blk_parts[:, SUM_ROW, SUM_LANE : SUM_LANE + 3 * groups].astype(F32), axis=0)
    shares = jnp.broadcast_to(pieces, (dp_count, pieces.shape[0]))
    shares = lax.all_to_all(shares, DP, split_axis=0, concat_axis=0, tiled=True)

    labels = jnp.arange(groups, dtype=jnp.int32)
    first = (labels == 0).astype(F32)
    onehot = (tile_group[..., None] == labels).astype(F32)
    counts = jnp.sum(onehot, axis=(0, 1, 2)) * float(block_height * block_cols) + first * float(
        tile_rows * mp_count * tile_cols * dp_count
    )
    blk_mom_t = jnp.transpose(blk_mom, (0, 2, 1, 3))
    emb_mom_t = jnp.transpose(emb_mom.reshape(dp_count, own_rows, tile_cols), (0, 2, 1))
    blk_shape = jax.ShapeDtypeStruct(blk_mom_t.shape, BF16)
    emb_shape = jax.ShapeDtypeStruct(emb_mom_t.shape, BF16)
    mixed = pl.pallas_call(
        mix_kernel,
        out_shape=blk_shape,
        in_specs=[ANY],
        out_specs=ANY,
        scratch_shapes=[
            pltpu.VMEM(packed.shape, BF16),
            pltpu.VMEM((block_cols // 128 + 1, matrices * owner_rows * mp_count, 128), F32),
            pltpu.VMEM(blk_mom_t.shape, BF16),
            pltpu.SemaphoreType.DMA(()),
            pltpu.SemaphoreType.DMA(()),
        ],
        compiler_params=pltpu.CompilerParams(vmem_limit_bytes=VMEM_BYTES),
        cost_estimate=pl.CostEstimate(flops=10_000_000, bytes_accessed=5_000_000, transcendentals=0),
        name="mix",
    )(blk_parts)

    early, late = EARLY, LATE
    n = len(early)
    payload, chunk = (EMB_ROWS, 128), emb_mom_t.shape[1:]
    emb_update, emb_moment, blk_update, blk_moment = pl.pallas_call(
        functools.partial(lion_kernel, early),
        out_shape=(emb_shape, emb_shape, blk_shape, blk_shape),
        in_specs=[SMEM] * 4 + [ANY] * (3 + n),
        out_specs=(ANY,) * 4,
        scratch_shapes=[pltpu.VMEM(blk_mom_t.shape, BF16)] * 2
        + [pltpu.VMEM((n,) + payload, BF16)]
        + [pltpu.VMEM((n,) + chunk, BF16)] * 3
        + [pltpu.VMEM(blk_mom_t.shape, BF16)] * 2
        + [pltpu.SemaphoreType.DMA((2 * (matrices + n),))] * 2,
        compiler_params=pltpu.CompilerParams(vmem_limit_bytes=VMEM_BYTES),
        cost_estimate=pl.CostEstimate(flops=30_000_000, bytes_accessed=25_000_000, transcendentals=0),
        name="lion",
    )(shares, counts, clip_rms, tile_group, mixed, blk_mom_t, emb_mom_t, *[emb_parts[i] for i in early])
    emb_update, emb_moment = pl.pallas_call(
        functools.partial(last_kernel, late),
        out_shape=(emb_shape, emb_shape),
        in_specs=[SMEM] * 3 + [ANY] * (3 + len(late)),
        out_specs=(ANY, ANY),
        scratch_shapes=[pltpu.VMEM((len(late),) + payload, BF16)]
        + [pltpu.VMEM((len(late),) + chunk, BF16)] * 3
        + [pltpu.SemaphoreType.DMA((2 * len(late),))] * 2,
        input_output_aliases={4 + len(late): 0, 5 + len(late): 1},
        compiler_params=pltpu.CompilerParams(vmem_limit_bytes=VMEM_BYTES),
        cost_estimate=pl.CostEstimate(flops=3_000_000, bytes_accessed=2_300_000, transcendentals=0),
        name="last",
    )(shares, counts, clip_rms, emb_mom_t, *[emb_parts[i] for i in late], emb_update, emb_moment)
    emb_update, emb_moment = (
        jnp.transpose(v, (0, 2, 1)).reshape(emb_mom.shape) for v in (emb_update, emb_moment)
    )
    return (
        emb_update,
        emb_moment,
        jnp.transpose(blk_update, (0, 2, 1, 3)),
        jnp.transpose(blk_moment, (0, 2, 1, 3)),
    )


EARLY = (7, 0, 3, 1, 5, 2, 4)
LATE = (6,)
FIRST = (0, 3)
REST = (1, 2, 4, 5, 6, 7)


def solution(mesh):
    torus = Mesh(mesh.devices.reshape(4, 2, 4, 2, 2), DP_MP)
    return jax.shard_map(
        on_device,
        mesh=torus,
        in_specs=(
            P(MP, DP),
            P(MP, None, DP, None, None),
            P(None, DP, MP),
            P(None, None, DP_MP, None),
            P(),
            P(),
        ),
        out_specs=(
            P(MP, None, DP, None, None),
            P(MP, None, DP, None, None),
            P(None, None, DP_MP, None),
            P(None, None, DP_MP, None),
        ),
        check_vma=False,
    )
```
